32 devices in a mesh: lat: 4 (over z), lon: 8 (over y, x, core).
Axes of the slice: x: 2, y: 2, z: 4, core: 2. Of those that a mesh axis runs over, the one named last changes fastest.
Arguments:
- grid_latent: bfloat16 [16384, 512], P(('lat', 'lon')), may hold values from -6 to 6
- mesh_latent: bfloat16 [4096, 512], P(('lat', 'lon')), may hold values from -6 to 6
- block_weights: bfloat16 [4, 3, 512, 512], replicated, may hold values from -0.25 to 0.25
- block_gains: float32 [4, 512], replicated, may hold values from 0.5 to 1.5
- grid_cot: bfloat16 [16384, 512], P(('lat', 'lon')), may hold values from -0.046875 to 0.046875
- encode_rows: int32 [32, 32, 4], P(('lat', 'lon')), may hold values from 0 to 511
- encode_senders: int32 [32, 1536], P(('lat', 'lon')), may hold values from 0 to 127, as said below
- encode_receivers: int32 [32, 1536], P(('lat', 'lon')), may hold values from 0 to 127, as said below
- encode_blocks: int32 [32], P(('lat', 'lon')), may hold values from 4 to 12, as said below
- process_rows: int32 [32, 32, 4], P(('lat', 'lon')), may hold values from 0 to 127
- process_senders: int32 [32, 1536], P(('lat', 'lon')), may hold values from 0 to 127, as said below
- process_receivers: int32 [32, 1536], P(('lat', 'lon')), may hold values from 0 to 127, as said below
- process_blocks: int32 [32], P(('lat', 'lon')), may hold values from 4 to 12, as said below
- decode_rows: int32 [32, 32, 4], P(('lat', 'lon')), may hold values from 0 to 127
- decode_senders: int32 [32, 1536], P(('lat', 'lon')), may hold values from 0 to 127, as said below
- decode_receivers: int32 [32, 1536], P(('lat', 'lon')), may hold values from 0 to 511, as said below
- decode_blocks: int32 [32], P(('lat', 'lon')), may hold values from 4 to 12, as said below
Outputs:
- grid_out: bfloat16 [16384, 512], P(('lat', 'lon'))
- weight_grad: bfloat16 [4, 3, 512, 512], replicated
- gain_grad: float32 [4, 512], replicated
The draws below stay inside these ranges and needn't reach their ends.
Inputs may be any that keep to these rules, and one draw needn't show every extreme that they name: `encode_senders`: on every device each of the 128 received slots is named by some edge of the first 4 blocks. `encode_receivers`: on every device each of its 128 mesh rows is named by some edge of the first 4 blocks. `encode_blocks`: some device has 12 live blocks. `process_senders`: on every device each of the 128 received slots is named by some edge of the first 4 blocks. `process_receivers`: on every device each of its 128 mesh rows is named by some edge of the first 4 blocks. `process_blocks`: some device has 12 live blocks. `decode_senders`: on every device each of the 128 received slots is named by some edge of the first 4 blocks. `decode_receivers`: on every device each of its 512 grid rows is named by some edge of the first 4 blocks. `decode_blocks`: some device has 12 live blocks.
All inputs are finite; a program needn't handle non-finite values.
Results may differ from the reference program's by a relative error of at most 0.017.
Values may be sent and summed in bfloat16 or wider, within the bound.
No kernel may reach another device: no remote copies, remote signals or barrier semaphores. Data moves between devices by JAX's collectives and lax.ppermute only.
A program may use at most 128 MiB of HBM per device.

```python
import jax
import jax.numpy as jnp
from jax import lax

D = 512
GRID_DEV = 512
MESH_DEV = 128
CAP = 4
LAYERS = 2
EDGE_BLOCK = 128
BLOCKS = 4
SLOTS = 128
MIN_BLK = 4
BLK = 12
EDGES = 1536
GRID = 16384
MESH = 4096
DEVICES = 32


def shuffled_row(one_key, limit):
    return jax.random.permutation(one_key, limit)


def cover_draw(key, salt, limit):
    base = jax.random.fold_in(key, salt)
    row_keys = jax.random.split(jax.random.fold_in(base, 1), DEVICES)
    shuffles = jax.vmap(lambda row_key: shuffled_row(row_key, limit))(row_keys).astype(jnp.int32)
    positions = jnp.arange(EDGES, dtype=jnp.int32)
    covered = shuffles[:, positions % limit]
    spread = jax.random.randint(jax.random.fold_in(base, 2), (DEVICES, EDGES), 0, limit, dtype=jnp.int32)
    return jnp.where(positions[None, :] < MIN_BLK * EDGE_BLOCK, covered, spread).astype(jnp.int32)


def count_draw(key, salt):
    base = jax.random.fold_in(key, salt)
    tries = jax.random.randint(jax.random.fold_in(base, 1), (3, DEVICES), 0, BLK - MIN_BLK + 1, dtype=jnp.int32)
    counts = MIN_BLK + jnp.min(tries, axis=0)
    busiest = jax.random.randint(jax.random.fold_in(base, 2), (), 0, DEVICES, dtype=jnp.int32)
    return jnp.where(jnp.arange(DEVICES, dtype=jnp.int32) == busiest, BLK, counts).astype(jnp.int32)


def draw_encode_senders(key, part):
    return cover_draw(key, 11, SLOTS)


def draw_encode_receivers(key, part):
    return cover_draw(key, 12, MESH_DEV)


def draw_encode_blocks(key, part):
    return count_draw(key, 13)


def draw_process_senders(key, part):
    return cover_draw(key, 21, SLOTS)


def draw_process_receivers(key, part):
    return cover_draw(key, 22, MESH_DEV)


def draw_process_blocks(key, part):
    return count_draw(key, 23)


def draw_decode_senders(key, part):
    return cover_draw(key, 31, SLOTS)


def draw_decode_receivers(key, part):
    return cover_draw(key, 32, GRID_DEV)


def draw_decode_blocks(key, part):
    return count_draw(key, 33)


def touch_ends(values, own_key, low, largest):
    shape = values.shape
    spot = [jax.random.randint(jax.random.fold_in(own_key, axis), (), 0, shape[axis]) for axis in range(len(shape))]
    values = values.at[tuple(spot)].set(low)
    longest = shape.index(max(shape))
    spot[longest] = (spot[longest] + 1) % shape[longest]
    return values.at[tuple(spot)].set(largest)


def block_levels(rng, extent, cuts, least, top_value):
    def one(axis_at, blocks):
        steps = jax.random.uniform(jax.random.fold_in(jax.random.fold_in(rng, 6), axis_at), (blocks,), jnp.float32, least / len(cuts), top_value / len(cuts))
        return jnp.repeat(jnp.exp(steps), extent[axis_at] // blocks).reshape((-1,) + (1,) * (len(extent) - axis_at - 1))

    gain = one(*cuts[0])
    for cut in cuts[1:]:
        gain = gain * one(*cut)
    return gain


def gaussian(key, shape, scale, most, shards=(), kind=jnp.bfloat16):
    entries = scale * jax.random.normal(key, shape, jnp.float32)
    if shards:
        entries = entries * block_levels(key, shape, shards, -0.22, 0.18)
    return jnp.clip(entries, -most, most).astype(kind)


def setup_inputs(seed: int = 0) -> dict:
    keys = jax.random.split(jax.random.key(seed), 18)
    return {
        "grid_latent": gaussian(keys[0], (GRID, D), 1.0, 6.0, ((0, 32),)),
        "mesh_latent": gaussian(keys[1], (MESH, D), 1.0, 6.0, ((0, 32),)),
        "block_weights": gaussian(keys[2], (BLOCKS, 3, D, D), D ** -0.5, 0.25),
        "block_gains": jnp.clip(1.0 + 0.1 * jax.random.normal(keys[3], (BLOCKS, D), jnp.float32), 0.5, 1.5),
        "grid_cot": gaussian(keys[4], (GRID, D), ((GRID_DEV * DEVICES) ** -0.5), 0.046875, ((0, 32),)),
        "encode_rows": touch_ends(jax.random.randint(keys[5], (DEVICES, DEVICES, CAP), 0, GRID_DEV), jax.random.fold_in(keys[5], 1), 0, GRID_DEV - 1).astype(jnp.int32),
        "encode_senders": draw_encode_senders(jax.random.fold_in(keys[17], 71), 0),
        "encode_receivers": draw_encode_receivers(jax.random.fold_in(keys[17], 71), 0),
        "encode_blocks": draw_encode_blocks(jax.random.fold_in(keys[17], 71), 0),
        "process_rows": touch_ends(jax.random.randint(keys[9], (DEVICES, DEVICES, CAP), 0, MESH_DEV), jax.random.fold_in(keys[9], 1), 0, MESH_DEV - 1).astype(jnp.int32),
        "process_senders": draw_process_senders(jax.random.fold_in(keys[17], 71), 0),
        "process_receivers": draw_process_receivers(jax.random.fold_in(keys[17], 71), 0),
        "process_blocks": draw_process_blocks(jax.random.fold_in(keys[17], 71), 0),
        "decode_rows": touch_ends(jax.random.randint(keys[13], (DEVICES, DEVICES, CAP), 0, MESH_DEV), jax.random.fold_in(keys[13], 1), 0, MESH_DEV - 1).astype(jnp.int32),
        "decode_senders": draw_decode_senders(jax.random.fold_in(keys[17], 71), 0),
        "decode_receivers": draw_decode_receivers(jax.random.fold_in(keys[17], 71), 0),
        "decode_blocks": draw_decode_blocks(jax.random.fold_in(keys[17], 71), 0),
    }


EPSILON = 1e-05

def silu_slope(values):
    sigma = jax.nn.sigmoid(values)
    return sigma * (1.0 + values * (1.0 - sigma))

def transposed_product(left, right):
    return lax.dot_general(left, right, (((0,), (0,)), ((), ())), preferred_element_type=jnp.float32)

def back_product(grad, weight):
    return lax.dot_general(grad, weight, (((1,), (1,)), ((), ())), preferred_element_type=jnp.float32)

def projected(latent, weight):
    return jnp.dot(latent, weight, preferred_element_type=jnp.float32).astype(jnp.bfloat16)

def edge_forward(slot_vals, proj_recv, latent_recv, senders, receivers, live_mask, weight_out, block_gain):
    preact = slot_vals[senders].astype(jnp.float32) + proj_recv[receivers].astype(jnp.float32)
    hidden = jax.nn.silu(preact) * live_mask[:, None]
    summed = jax.ops.segment_sum(hidden, receivers, num_segments=proj_recv.shape[0]).astype(jnp.bfloat16)
    mixed = jnp.dot(summed, weight_out, preferred_element_type=jnp.float32)
    centred = mixed - lax.optimization_barrier(jnp.mean(mixed, axis=-1, keepdims=True))
    inv_scale = lax.rsqrt(lax.optimization_barrier(jnp.mean(centred * centred, axis=-1, keepdims=True)) + EPSILON)
    normed = centred * inv_scale
    output = (latent_recv.astype(jnp.float32) + normed * block_gain).astype(jnp.bfloat16)
    return (output, preact, summed, normed, inv_scale)

def edge_backward(grad_out, preact, summed, normed, inv_scale, senders, receivers, live_mask, weight_out, block_gain, recv_count, slot_count):
    gain_part = lax.optimization_barrier(jnp.sum(grad_out * normed, axis=0))
    grad_normed = grad_out * block_gain
    grad_mixed = inv_scale * (grad_normed - lax.optimization_barrier(jnp.mean(grad_normed, axis=-1, keepdims=True)) - normed * lax.optimization_barrier(jnp.mean(grad_normed * normed, axis=-1, keepdims=True)))
    grad_mixed = grad_mixed.astype(jnp.bfloat16)
    out_part = transposed_product(summed, grad_mixed)
    grad_summed = back_product(grad_mixed, weight_out)
    grad_pre = grad_summed[receivers] * live_mask[:, None] * silu_slope(preact)
    grad_recv = jax.ops.segment_sum(grad_pre, receivers, num_segments=recv_count).astype(jnp.bfloat16)
    grad_slots = jax.ops.segment_sum(grad_pre, senders, num_segments=slot_count).astype(jnp.bfloat16)
    return (grad_recv, grad_slots, out_part, gain_part)

def slot_table(send_rows, stride):
    offsets = jnp.arange(send_rows.shape[0], dtype=jnp.int32) * stride
    table = jnp.transpose(send_rows, (1, 0, 2)) + offsets[None, :, None]
    return table.reshape(send_rows.shape[0], -1).astype(jnp.int32)

def live_table(block_count):
    positions = jnp.arange(EDGES, dtype=jnp.int32) // EDGE_BLOCK
    return (positions[None, :] < block_count[:, None]).astype(jnp.float32)

def block_forward(latent_send, latent_recv, weights, block_gain, graph, stride):
    send_rows, senders, receivers, block_count = graph
    proj_send = projected(latent_send, weights[0])
    proj_recv = projected(latent_recv, weights[1])
    table = slot_table(send_rows, stride)
    live = live_table(block_count)

    def one_device(pieces):
        table_row, proj_part, latent_part, send_part, recv_part, live_part = pieces
        return edge_forward(proj_send[table_row], proj_part, latent_part, send_part, recv_part, live_part, weights[2], block_gain)[0]
    outputs = lax.map(one_device, (table, proj_recv.reshape(DEVICES, -1, D), latent_recv.reshape(DEVICES, -1, D), senders, receivers, live))
    return outputs.reshape(-1, D)

def block_backward(grad_out, latent_send, latent_recv, weights, block_gain, graph, stride):
    send_rows, senders, receivers, block_count = graph
    proj_send = projected(latent_send, weights[0])
    proj_recv = projected(latent_recv, weights[1])
    table = slot_table(send_rows, stride)
    live = live_table(block_count)

    def one_device(carry, pieces):
        table_row, proj_part, latent_part, send_part, recv_part, live_part, grad_part = pieces
        slot_vals = proj_send[table_row]
        output, preact, summed, normed, inv_scale = edge_forward(slot_vals, proj_part, latent_part, send_part, recv_part, live_part, weights[2], block_gain)
        grad_recv, grad_slots, out_part, gain_part = edge_backward(grad_part, preact, summed, normed, inv_scale, send_part, recv_part, live_part, weights[2], block_gain, proj_part.shape[0], slot_vals.shape[0])
        return ((carry[0] + out_part, carry[1] + gain_part), (grad_recv, grad_slots))
    start = (jnp.zeros((D, D), jnp.float32), jnp.zeros((D,), jnp.float32))
    stacked = (table, proj_recv.reshape(DEVICES, -1, D), latent_recv.reshape(DEVICES, -1, D), senders, receivers, live, grad_out.reshape(DEVICES, -1, D))
    (grad_wout, gain_total), (grad_recv, grad_slots) = lax.scan(one_device, start, stacked)
    grad_recv = grad_recv.reshape(-1, D)
    grad_send = jax.ops.segment_sum(grad_slots.reshape(-1, D).astype(jnp.float32), table.reshape(-1), num_segments=latent_send.shape[0]).astype(jnp.bfloat16)
    grad_weights = jnp.stack([transposed_product(latent_send, grad_send), transposed_product(latent_recv, grad_recv), grad_wout])
    return (grad_weights, gain_total, back_product(grad_send, weights[0]), back_product(grad_recv, weights[1]))

def reference(grid_latent, mesh_latent, block_weights, block_gains, grid_cot, encode_rows, encode_senders, encode_receivers, encode_blocks, process_rows, process_senders, process_receivers, process_blocks, decode_rows, decode_senders, decode_receivers, decode_blocks):
    encode = (encode_rows, encode_senders, encode_receivers, encode_blocks)
    process = (process_rows, process_senders, process_receivers, process_blocks)
    decode = (decode_rows, decode_senders, decode_receivers, decode_blocks)
    latents = [mesh_latent]
    latents.append(block_forward(grid_latent, mesh_latent, block_weights[0], block_gains[0], encode, GRID_DEV))
    for layer_id in range(LAYERS):
        current = latents[-1]
        latents.append(block_forward(current, current, block_weights[layer_id + 1], block_gains[layer_id + 1], process, MESH_DEV))
    last_id = LAYERS + 1
    grid_out = block_forward(latents[-1], grid_latent, block_weights[last_id], block_gains[last_id], decode, MESH_DEV)
    weight_parts = [None] * (LAYERS + 2)
    gain_parts = [None] * (LAYERS + 2)
    grad_weights, gain_total, down_send, down_recv = block_backward(grid_cot.astype(jnp.float32), latents[-1], grid_latent, block_weights[last_id], block_gains[last_id], decode, MESH_DEV)
    weight_parts[last_id] = grad_weights
    gain_parts[last_id] = gain_total
    grad_mesh = down_send
    for layer_id in reversed(range(LAYERS)):
        block_id = layer_id + 1
        current = latents[block_id]
        grad_weights, gain_total, down_send, down_recv = block_backward(grad_mesh, current, current, block_weights[block_id], block_gains[block_id], process, MESH_DEV)
        weight_parts[block_id] = grad_weights
        gain_parts[block_id] = gain_total
        grad_mesh = grad_mesh + down_recv + down_send
    grad_weights, gain_total, down_send, down_recv = block_backward(grad_mesh, grid_latent, mesh_latent, block_weights[0], block_gains[0], encode, GRID_DEV)
    weight_parts[0] = grad_weights
    gain_parts[0] = gain_total
    return (grid_out, jnp.stack(weight_parts).astype(jnp.bfloat16), jnp.stack(gain_parts))
```

```python
import functools

import jax
import jax.numpy as jnp
from jax import lax
from jax.experimental import pallas as pl
from jax.experimental.pallas import tpu as pltpu
from jax.sharding import PartitionSpec as P

LAYERS = 2
EDGE_BLOCK = 128
EPSILON = 1e-05
LANES = 128
CHUNK = 256
AXES = ("lat", "lon")
F32 = jnp.float32
BF16 = jnp.bfloat16


def dot(left, right):
    return jnp.dot(left, right, preferred_element_type=F32)


def dot_left_t(left, right):
    return lax.dot_general(left, right, (((0,), (0,)), ((), ())), preferred_element_type=F32)


def dot_right_t(left, right):
    return lax.dot_general(left, right, (((1,), (1,)), ((), ())), preferred_element_type=F32)


def call(body, outs, args, scratch=(), flops=0, smem=(), vmem=None):
    specs = [
        pl.BlockSpec(memory_space=pltpu.SMEM if i in smem else pltpu.VMEM)
        for i in range(len(args))
    ]
    return pl.pallas_call(
        body,
        out_shape=[jax.ShapeDtypeStruct(shape, kind) for shape, kind in outs],
        in_specs=specs,
        out_specs=[pl.BlockSpec(memory_space=pltpu.VMEM)] * len(outs),
        scratch_shapes=list(scratch),
        cost_estimate=pl.CostEstimate(flops=flops, bytes_accessed=0, transcendentals=0),
        compiler_params=pltpu.CompilerParams(vmem_limit_bytes=vmem or 24 * 1024 * 1024),
    )(*args)


def ones_where(mask):
    return jnp.where(mask, 1.0, 0.0).astype(BF16)


def pick_down(row, count):
    steps = lax.broadcasted_iota(jnp.int32, (count, row.shape[1]), 0)
    return ones_where(steps == row)


def pick_across(row, count):
    n = row.shape[1]
    column = jnp.transpose(jnp.broadcast_to(row, (LANES, n)))
    steps = lax.broadcasted_iota(jnp.int32, (n, LANES), 1)
    pieces = [ones_where(column == steps + base) for base in range(0, count, LANES)]
    return jnp.concatenate(pieces, axis=1)


def stack_lanes(value):
    return jnp.concatenate(
        [value[:, i : i + LANES] for i in range(0, value.shape[1], LANES)], axis=0
    )


def spread_lanes(value, rows):
    return jnp.concatenate(
        [value[i : i + rows] for i in range(0, value.shape[0], rows)], axis=1
    )


def pack_order(rows, blocks, cap):
    total = rows * blocks
    place = lax.broadcasted_iota(jnp.int32, (total, 1), 0)
    group = place // (blocks * cap)
    block = (place // cap) % blocks
    want = block * rows + group * cap + place % cap
    return ones_where(lax.broadcasted_iota(jnp.int32, (total, total), 1) == want)


def unpack_order(rows, blocks, cap):
    total = rows * blocks
    place = lax.broadcasted_iota(jnp.int32, (total, 1), 0)
    block = place // rows
    inner = place % rows
    want = (inner // cap) * (blocks * cap) + block * cap + inner % cap
    return ones_where(lax.broadcasted_iota(jnp.int32, (total, total), 1) == want)


def pack(value, cap):
    rows, width = value.shape
    order = pack_order(rows, width // LANES, cap)
    return dot(order, stack_lanes(value)).astype(BF16)


def unpack(value, rows, cap):
    order = unpack_order(rows, value.shape[0] // rows, cap)
    return spread_lanes(dot(order, value), rows).astype(BF16)


def first_body(cap, rows_ref, latent_ref, out_ref):
    picks = pick_across(rows_ref[...], latent_ref.shape[0])
    out_ref[...] = pack(dot(picks, latent_ref[...]).astype(BF16), cap)


def prep_body(slots, recv, senders_ref, receivers_ref, blocks_ref, across_ref, down_ref):
    edges = senders_ref.shape[1]
    place = lax.broadcasted_iota(jnp.int32, (1, edges), 1)
    alive = place < blocks_ref[0] * EDGE_BLOCK
    senders = senders_ref[...]
    receivers = jnp.where(alive, receivers_ref[...], -1)
    across_ref[:, :slots] = pick_across(senders, slots)
    across_ref[:, slots:] = pick_across(receivers, recv)
    down_ref[:slots] = pick_down(senders, slots)
    down_ref[slots:] = pick_down(receivers, recv)


def project_body(latent_ref, weight_ref, out_ref):
    out_ref[...] = dot(latent_ref[...], weight_ref[...]).astype(BF16)


def edge_pass(table, across_ref, down_ref, slots, hidden_ref, slope_ref):
    edges = across_ref.shape[0]
    for start in range(0, edges, CHUNK):
        span = pl.ds(start, CHUNK)
        preact = dot(across_ref[span], table)
        sigma = 0.5 * jnp.tanh(0.5 * preact) + 0.5
        hidden = preact * sigma
        hidden_ref[span] = hidden.astype(BF16)
        slope_ref[span] = (sigma + hidden * (1.0 - sigma)).astype(BF16)
    return dot(down_ref[slots:], hidden_ref[...]).astype(BF16)


def norm_pass(summed, weight_out):
    mixed = dot(summed, weight_out)
    centred = mixed - jnp.mean(mixed, axis=-1, keepdims=True)
    inv_scale = lax.rsqrt(jnp.mean(centred * centred, axis=-1, keepdims=True) + EPSILON)
    return centred * inv_scale, inv_scale


def forward_body(
    cap,
    arrived_ref,
    proj_ref,
    latent_ref,
    across_ref,
    down_ref,
    rows_ref,
    w_send_ref,
    w_out_ref,
    gain_ref,
    latent_out_ref,
    packed_ref,
    slot_ref,
    summed_ref,
    normed_ref,
    inv_ref,
    slope_ref,
    hidden_ref,
):
    slots = across_ref.shape[1] - latent_ref.shape[0]
    slot_latent = unpack(arrived_ref[...], slots, cap)
    slot_ref[...] = slot_latent
    slot_proj = dot(slot_latent, w_send_ref[...]).astype(BF16)
    table = jnp.concatenate([slot_proj, proj_ref[...]], axis=0)
    summed = edge_pass(table, across_ref, down_ref, slots, hidden_ref, slope_ref)
    summed_ref[...] = summed
    normed, inv_scale = norm_pass(summed, w_out_ref[...])
    normed_ref[...] = normed
    inv_ref[...] = inv_scale
    output = (latent_ref[...].astype(F32) + normed * gain_ref[...]).astype(BF16)
    latent_out_ref[...] = output
    picks = pick_across(rows_ref[...], output.shape[0])
    packed_ref[...] = pack(dot(picks, output).astype(BF16), cap)


def backward_pass(
    cap,
    grad_out,
    normed,
    inv_scale,
    gain,
    w_out,
    across_ref,
    down_ref,
    slope_ref,
    work_ref,
    packed_ref,
    grad_slots_ref,
    grad_recv_ref,
    grad_mixed_ref,
    gain_part_ref,
):
    slots = grad_slots_ref.shape[0]
    gain_part_ref[...] = jnp.sum(grad_out * normed, axis=0, keepdims=True)
    grad_normed = grad_out * gain
    grad_mixed = inv_scale * (
        grad_normed
        - jnp.mean(grad_normed, axis=-1, keepdims=True)
        - normed * jnp.mean(grad_normed * normed, axis=-1, keepdims=True)
    )
    grad_mixed = grad_mixed.astype(BF16)
    grad_mixed_ref[...] = grad_mixed
    grad_summed = dot_right_t(grad_mixed, w_out).astype(BF16)
    edges = across_ref.shape[0]
    for start in range(0, edges, CHUNK):
        span = pl.ds(start, CHUNK)
        grad_edge = dot(across_ref[span, slots:], grad_summed)
        work_ref[span] = (grad_edge * slope_ref[span].astype(F32)).astype(BF16)
    grad_slots = dot(down_ref[:slots], work_ref[...]).astype(BF16)
    grad_slots_ref[...] = grad_slots
    if packed_ref is not None:
        packed_ref[...] = pack(grad_slots, cap)
    grad_recv_ref[...] = dot(down_ref[slots:], work_ref[...]).astype(BF16)


def last_body(
    cap,
    arrived_ref,
    proj_ref,
    latent_ref,
    across_ref,
    down_ref,
    w_send_ref,
    w_out_ref,
    gain_ref,
    cot_ref,
    latent_out_ref,
    packed_ref,
    slot_ref,
    summed_ref,
    grad_slots_ref,
    grad_recv_ref,
    grad_mixed_ref,
    gain_part_ref,
    slope_ref,
    hidden_ref,
):
    slots = across_ref.shape[1] - latent_ref.shape[0]
    slot_latent = unpack(arrived_ref[...], slots, cap)
    slot_ref[...] = slot_latent
    slot_proj = dot(slot_latent, w_send_ref[...]).astype(BF16)
    table = jnp.concatenate([slot_proj, proj_ref[...]], axis=0)
    summed = edge_pass(table, across_ref, down_ref, slots, hidden_ref, slope_ref)
    summed_ref[...] = summed
    normed, inv_scale = norm_pass(summed, w_out_ref[...])
    gain = gain_ref[...]
    latent_out_ref[...] = (latent_ref[...].astype(F32) + normed * gain).astype(BF16)
    backward_pass(
        cap,
        cot_ref[...].astype(F32),
        normed,
        inv_scale,
        gain,
        w_out_ref[...],
        across_ref,
        down_ref,
        slope_ref,
        hidden_ref,
        packed_ref,
        grad_slots_ref,
        grad_recv_ref,
        grad_mixed_ref,
        gain_part_ref,
    )


def backward_body(
    cap,
    has_base,
    sends,
    arrived_ref,
    rows_ref,
    w_next_ref,
    base_ref,
    normed_ref,
    inv_ref,
    gain_ref,
    w_out_ref,
    across_ref,
    down_ref,
    slope_ref,
    grad_send_ref,
    *rest,
):
    if sends:
        packed_ref, grad_slots_ref, grad_recv_ref, grad_mixed_ref, gain_part_ref, grad_mesh_ref, work_ref = rest
    else:
        packed_ref = None
        grad_slots_ref, grad_recv_ref, grad_mixed_ref, gain_part_ref, grad_mesh_ref, work_ref = rest
    returned = unpack(arrived_ref[...], rows_ref.shape[1], cap)
    picks = pick_down(rows_ref[...], normed_ref.shape[0])
    grad_send = dot(picks, returned).astype(BF16)
    grad_send_ref[...] = grad_send
    grad_mesh = dot_right_t(grad_send, w_next_ref[...])
    if has_base:
        grad_mesh = grad_mesh + base_ref[...]
    grad_mesh_ref[...] = grad_mesh
    backward_pass(
        cap,
        grad_mesh,
        normed_ref[...],
        inv_ref[...],
        gain_ref[...],
        w_out_ref[...],
        across_ref,
        down_ref,
        slope_ref,
        work_ref,
        packed_ref,
        grad_slots_ref,
        grad_recv_ref,
        grad_mixed_ref,
        gain_part_ref,
    )


def stages_of(count):
    bits = count.bit_length() - 1
    fields = [(0, 1)] if bits else []
    at = 1
    while at < bits:
        width = min(2, bits - at)
        fields.append((at, width))
        at += width
    return fields


def slot_of(relative, count):
    place = relative * 0
    left = count
    for at, width in stages_of(count):
        left = left >> width
        place = place + ((relative >> at) & ((1 << width) - 1)) * left
    return place


def weight_body(
    count,
    has_next,
    me_ref,
    slot_ref,
    grad_slots_ref,
    latent_ref,
    grad_recv_ref,
    summed_ref,
    grad_mixed_ref,
    grad_mesh_ref,
    w_recv_ref,
    *rest,
):
    if has_next:
        own_ref, send_ref, next_ref, work_ref = rest
    else:
        own_ref, send_ref, work_ref = rest
    me = me_ref[0]
    parts = [
        dot_left_t(slot_ref[...], grad_slots_ref[...]),
        dot_left_t(latent_ref[...], grad_recv_ref[...]),
        dot_left_t(summed_ref[...], grad_mixed_ref[...]),
    ]
    whole = jnp.concatenate(parts, axis=0).astype(BF16)
    rows = work_ref.shape[1]
    for chunk in range(count):
        work_ref[slot_of(me ^ chunk, count)] = whole[chunk * rows : (chunk + 1) * rows]
    own_ref[...] = work_ref[: count // 2]
    send_ref[...] = work_ref[count // 2 :]
    if has_next:
        next_ref[...] = grad_mesh_ref[...] + dot_right_t(grad_recv_ref[...], w_recv_ref[...])


def merge_body(ways, *refs):
    total = refs[0][...].astype(F32)
    for i in range(1, ways):
        total = total + refs[i][...].astype(F32)
    total = total.astype(BF16)
    outs = refs[ways:]
    size = outs[0].shape[0]
    for i, out in enumerate(outs):
        out[...] = total[i * size : (i + 1) * size]


def final_body(count, me_ref, *refs):
    pieces, out_ref, work_ref = refs[:-2], refs[-2], refs[-1]
    at = 0
    for piece in pieces:
        size = piece.shape[0]
        work_ref[at : at + size] = piece[...]
        at += size
    me = me_ref[0]
    rows = work_ref.shape[1]
    for chunk in range(count):
        out_ref[chunk * rows : (chunk + 1) * rows] = work_ref[slot_of(me ^ chunk, count)]


def swap(value, mask, count):
    return lax.ppermute(value, AXES, [(i, i ^ mask) for i in range(count)])


def reduce_stages(own, send, count):
    fields = stages_of(count)
    pieces = [own, swap(send, 1, count)]
    for at, width in fields[1:]:
        ways = 1 << width
        size = pieces[0].shape[0] // ways
        shape = (size,) + pieces[0].shape[1:]
        split = call(
            functools.partial(merge_body, len(pieces)), [(shape, BF16)] * ways, pieces
        )
        pieces = [split[0]] + [swap(split[i], i << at, count) for i in range(1, ways)]
    return call(
        functools.partial(merge_body, len(pieces)), [(pieces[0].shape, BF16)], pieces
    )[0]


def gather_stages(chunk, me, count):
    pieces = [chunk]
    fields = stages_of(count)
    for at, width in reversed(fields):
        held = jnp.concatenate(pieces, axis=0) if len(pieces) > 1 else pieces[0]
        pieces = [held] + [swap(held, i << at, count) for i in range(1, 1 << width)]
    rows, width = chunk.shape[1:]
    return call(
        functools.partial(final_body, count),
        [((count * rows, width), BF16)],
        [me] + pieces,
        scratch=[pltpu.VMEM((count, rows, width), BF16)],
        smem=(0,),
    )[0]


def trade(packed, count):
    spread = packed.reshape(count, -1, packed.shape[1])
    back = lax.all_to_all(spread, AXES, split_axis=0, concat_axis=0, tiled=True)
    return back.reshape(packed.shape)


def shards(
    count,
    grid_latent,
    mesh_latent,
    block_weights,
    block_gains,
    grid_cot,
    encode_rows,
    encode_senders,
    encode_receivers,
    encode_blocks,
    process_rows,
    process_senders,
    process_receivers,
    process_blocks,
    decode_rows,
    decode_senders,
    decode_receivers,
    decode_blocks,
):
    width = grid_latent.shape[1]
    grid_count = grid_latent.shape[0]
    mesh_count = mesh_latent.shape[0]
    cap = encode_rows.shape[2]
    slots = encode_rows.shape[1] * cap
    edges = encode_senders.shape[1]
    packed_shape = (slots * width // LANES, LANES)
    last_id = LAYERS + 1
    me = (lax.axis_index("lat") * lax.axis_size("lon") + lax.axis_index("lon")).reshape(1)
    rows = [r.reshape(1, slots) for r in (encode_rows, process_rows, decode_rows)]
    weights = [[block_weights[b, i] for i in range(3)] for b in range(last_id + 1)]
    gains = [block_gains[b : b + 1] for b in range(last_id + 1)]

    packed = call(
        functools.partial(first_body, cap),
        [(packed_shape, BF16)],
        [rows[0], grid_latent],
        flops=2 * slots * width * (grid_count + slots),
    )[0]
    arrived = trade(packed, count)

    graphs = []
    for senders, receivers, blocks, recv in (
        (encode_senders, encode_receivers, encode_blocks, mesh_count),
        (process_senders, process_receivers, process_blocks, mesh_count),
        (decode_senders, decode_receivers, decode_blocks, grid_count),
    ):
        graphs.append(
            call(
                functools.partial(prep_body, slots, recv),
                [((edges, slots + recv), BF16), ((slots + recv, edges), BF16)],
                [senders, receivers, blocks],
                smem=(2,),
                flops=10**9,
            )
        )
    block_graphs = [graphs[0]] + [graphs[1]] * LAYERS + [graphs[2]]
    block_rows = [rows[0]] + [rows[1]] * LAYERS + [rows[2]]

    def project(latent, weight):
        return call(
            project_body,
            [(latent.shape, BF16)],
            [latent, weight],
            flops=2 * latent.shape[0] * width * width,
        )[0]

    recv_latents = [mesh_latent]
    saves = []
    for b in range(last_id):
        latent = recv_latents[b]
        across, down = block_graphs[b]
        proj = project(latent, weights[b][1])
        latent_out, packed, slot_latent, summed, normed, inv, slope = call(
            functools.partial(forward_body, cap),
            [
                ((mesh_count, width), BF16),
                (packed_shape, BF16),
                ((slots, width), BF16),
                ((mesh_count, width), BF16),
                ((mesh_count, width), F32),
                ((mesh_count, 1), F32),
                ((edges, width), BF16),
            ],
            [
                arrived,
                proj,
                latent,
                across,
                down,
                block_rows[b + 1],
                weights[b][0],
                weights[b][2],
                gains[b],
            ],
            scratch=[pltpu.VMEM((edges, width), BF16)],
            flops=2 * 10**9,
        )
        recv_latents.append(latent_out)
        saves.append((slot_latent, summed, normed, inv, slope))
        arrived = trade(packed, count)
    recv_latents[last_id] = grid_latent
    proj = project(grid_latent, weights[last_id][1])
    across, down = graphs[2]
    grid_out, packed, slot_latent, summed, grad_slots, grad_recv, grad_mixed, gain_part = call(
        functools.partial(last_body, cap),
        [
            ((grid_count, width), BF16),
            (packed_shape, BF16),
            ((slots, width), BF16),
            ((grid_count, width), BF16),
            ((slots, width), BF16),
            ((grid_count, width), BF16),
            ((grid_count, width), BF16),
            ((1, width), F32),
        ],
        [
            arrived,
            proj,
            grid_latent,
            across,
            down,
            weights[last_id][0],
            weights[last_id][2],
            gains[last_id],
            grid_cot,
        ],
        scratch=[pltpu.VMEM((edges, width), BF16)] * 2,
        flops=8 * 10**9,
        vmem=32 * 1024 * 1024,
    )

    chunk_rows = 3 * width // count

    def weight_parts(b, slot_latent, summed, grads, grad_mesh):
        grad_slots, grad_recv, grad_mixed = grads
        half = (count // 2, chunk_rows, width)
        has_next = 0 < b < last_id
        outs = [(half, BF16), (half, BF16)]
        if has_next:
            outs.append((grad_mesh.shape, F32))
        return call(
            functools.partial(weight_body, count, has_next),
            outs,
            [
                me,
                slot_latent,
                grad_slots,
                recv_latents[b],
                grad_recv,
                summed,
                grad_mixed,
                grad_mesh,
                weights[b][1],
            ],
            scratch=[pltpu.VMEM((count, chunk_rows, width), BF16)],
            smem=(0,),
            flops=10**9,
        )

    gain_parts = [None] * (last_id + 1)
    totals = [None] * (last_id + 1)
    gain_parts[last_id] = gain_part
    arrived = trade(packed, count)
    dummy = jnp.zeros((8, LANES), F32)
    own, send = weight_parts(
        last_id, slot_latent, summed, (grad_slots, grad_recv, grad_mixed), dummy
    )
    totals[last_id] = gather_stages(reduce_stages(own, send, count), me, count)
    base = dummy
    for b in reversed(range(last_id)):
        slot_latent, summed, normed, inv, slope = saves[b]
        across, down = block_graphs[b]
        sends = b > 0
        outs = [((mesh_count, width), BF16)]
        if sends:
            outs.append((packed_shape, BF16))
        outs += [
            ((slots, width), BF16),
            ((mesh_count, width), BF16),
            ((mesh_count, width), BF16),
            ((1, width), F32),
            ((mesh_count, width), F32),
        ]
        results = call(
            functools.partial(backward_body, cap, b < last_id - 1, sends),
            outs,
            [
                arrived,
                block_rows[b + 1],
                weights[b + 1][0],
                base,
                normed,
                inv,
                gains[b],
                weights[b][2],
                across,
                down,
                slope,
            ],
            scratch=[pltpu.VMEM((edges, width), BF16)],
            flops=2 * 10**9,
        )
        grad_slots, grad_recv, grad_mixed, gain_part, grad_mesh = results[-5:]
        gain_parts[b] = gain_part
        if sends:
            arrived = trade(results[1], count)
        parts = weight_parts(b, slot_latent, summed, (grad_slots, grad_recv, grad_mixed), grad_mesh)
        if sends:
            own, send, base = parts
        else:
            own, send = parts
        totals[b] = gather_stages(reduce_stages(own, send, count), me, count)
    gain_stack = lax.psum(jnp.concatenate(gain_parts, axis=0), AXES)
    weight_stack = jnp.stack(totals).reshape(block_weights.shape)
    return (grid_out, weight_stack, gain_stack)


def solution(mesh):
    count = mesh.shape["lat"] * mesh.shape["lon"]
    wide = P(AXES, None)
    graph = (P(AXES, None, None), wide, wide, P(AXES))
    return jax.shard_map(
        functools.partial(shards, count),
        mesh=mesh,
        in_specs=(wide, wide, P(), P(), wide) + graph * 3,
        out_specs=(wide, P(), P()),
        check_vma=False,
    )
```
